32 devices in a mesh: gx: 4 (over y, core), gy: 4 (over z), gz: 2 (over x).
Axes of the slice: x: 2, y: 2, z: 4, core: 2. Of those that a mesh axis runs over, the one named last changes fastest.
Arguments:
- permittivity: float32 [32, 128, 256], P('gx', 'gy', 'gz'), may hold values from 1 to 9
- loss: float32 [32, 128, 256], P('gx', 'gy', 'gz'), may hold values from 0 to 0.2
- fwd_electric: float32 [3, 32, 128, 256], P(None, 'gx', 'gy', 'gz'), may hold values from -6 to 6
- fwd_magnetic: float32 [3, 32, 128, 256], P(None, 'gx', 'gy', 'gz'), may hold values from -6 to 6
- adj_electric: float32 [3, 32, 128, 256], P(None, 'gx', 'gy', 'gz'), may hold values from -200 to 200
- adj_magnetic: float32 [3, 32, 128, 256], P(None, 'gx', 'gy', 'gz'), may hold values from -200 to 200
- wavelet: float32 [64], replicated, may hold values from -6 to 6
- residuals: float32 [256, 64], P(('gx', 'gy', 'gz')), may hold values from -24 to 24
- source_cell: int32 [1], replicated, may hold values from 0 to 1048575
- receiver_cells: int32 [256], replicated, may hold values from 0 to 1048575
- start_step: int32 [1], replicated, may hold values from 0 to 60
Outputs:
- direction: float32 [32, 128, 256], P('gx', 'gy', 'gz')
- grad_rms: float32 [], replicated
The draws below stay inside these ranges and needn't reach their ends.
Inputs may be any that keep to these rules, and one draw needn't show every extreme that they name: source_cell[0] is a flat index of a cell. receiver_cells[r] is the flat index of receiver r's cell; several receivers may share a cell. Samples start_step to start_step + 3 exist in every trace.
All inputs are finite; a program needn't handle non-finite values.
Results may differ from the reference program's by a relative error of at most 0.0003.
Values sent between devices are 32-bit elements; how exact they have to be, the bound alone decides.
A program may use at most 128 MiB of HBM per device.

```python
import math
import jax
import jax.numpy as jnp
from jax import lax

STEPS = 4
TRACE = 64
NREC = 256
NX = 32
NY = 128
NZ = 256


def adjoint_field(key):
    keys = jax.random.split(key, 4)
    ramp = 3.0 ** (jnp.arange(NX, dtype=jnp.float32) / NX)
    scale_x = ramp
    scale_y = jnp.exp(jax.random.uniform(keys[2], (NY,), jnp.float32, 0.0, math.log(4.0)))
    scale_z = jnp.exp(jax.random.uniform(keys[3], (NZ,), jnp.float32, 0.0, math.log(2.0)))
    base = jnp.clip(jax.random.normal(keys[0], (3, NX, NY, NZ), jnp.float32), -6.0, 6.0)
    return base * scale_x[None, :, None, None] * scale_y[None, None, :, None] * scale_z[None, None, None, :]


def draw_adj_electric(key, part):
    return adjoint_field(jax.random.fold_in(key, 11))


def draw_adj_magnetic(key, part):
    return adjoint_field(jax.random.fold_in(key, 23))


def place_ends(values, rng, low, high):
    longest = values.shape.index(max(values.shape))
    spots = []
    for shift in (0, 1):
        where = [jax.random.randint(jax.random.fold_in(rng, axis), (), 0, length) for axis, length in enumerate(values.shape)]
        where[longest] = (where[longest] + shift) % values.shape[longest]
        spots.append(tuple(where))
    return values.at[spots[0]].set(low).at[spots[1]].set(high)


def levels(stream_key, shape, cuts, low, largest):
    def one(dim, parts):
        steps = jax.random.uniform(jax.random.fold_in(jax.random.fold_in(stream_key, 6), dim), (parts,), jnp.float32, low / len(cuts), largest / len(cuts))
        return jnp.repeat(jnp.exp(steps), shape[dim] // parts).reshape((-1,) + (1,) * (len(shape) - dim - 1))

    gain = one(*cuts[0])
    for cut in cuts[1:]:
        gain = gain * one(*cut)
    return gain


def normal_values(stream_key, dims, spread, limit, shards=(), kind=jnp.bfloat16):
    values = spread * jax.random.normal(stream_key, dims, jnp.float32)
    if shards:
        values = values * levels(stream_key, dims, shards, -0.22, 0.18)
    return jnp.clip(values, -limit, limit).astype(kind)


def setup_inputs(seed: int = 0) -> dict:
    seeds = jax.random.split(jax.random.key(seed), 12)
    return {
        "permittivity": jnp.clip(jnp.exp(math.log(9.0) - 2.1972246 * jax.random.uniform(seeds[0], (NX, NY, NZ), jnp.float32) ** levels(seeds[0], (NX, NY, NZ), ((0, 4), (1, 4), (2, 2)), -0.2, 0.2)), 1.0, 9.0),
        "loss": jnp.clip(0.2 * jax.random.uniform(seeds[1], (NX, NY, NZ), jnp.float32) ** levels(seeds[1], (NX, NY, NZ), ((0, 4), (1, 4), (2, 2)), -0.2, 0.2), 0.0, 0.2),
        "fwd_electric": normal_values(seeds[2], (3, NX, NY, NZ), 1.0, 6.0, ((1, 4), (2, 4), (3, 2)), jnp.float32),
        "fwd_magnetic": normal_values(seeds[3], (3, NX, NY, NZ), 1.0, 6.0, ((1, 4), (2, 4), (3, 2)), jnp.float32),
        "adj_electric": draw_adj_electric(jax.random.fold_in(seeds[11], 71), 0),
        "adj_magnetic": draw_adj_magnetic(jax.random.fold_in(seeds[11], 71), 0),
        "wavelet": normal_values(seeds[6], (TRACE,), 1.0, 6.0, (), jnp.float32),
        "residuals": normal_values(seeds[7], (NREC, TRACE), 4.0, 24.0, ((0, 32),), jnp.float32),
        "source_cell": jax.random.randint(seeds[8], (1,), 0, NX * NY * NZ).astype(jnp.int32),
        "receiver_cells": place_ends(jax.random.randint(seeds[9], (NREC,), 0, NX * NY * NZ), jax.random.fold_in(seeds[9], 1), 0, (NX * NY * NZ) - 1).astype(jnp.int32),
        "start_step": jax.random.randint(seeds[10], (1,), 0, TRACE - STEPS + 1).astype(jnp.int32),
    }


def shifted_above(field, axis):
    rest = lax.slice_in_dim(field, 1, field.shape[axis], axis=axis)
    edge = jnp.zeros_like(lax.slice_in_dim(field, 0, 1, axis=axis))
    return jnp.concatenate([rest, edge], axis)

def shifted_below(field, axis):
    rest = lax.slice_in_dim(field, 0, field.shape[axis] - 1, axis=axis)
    edge = jnp.zeros_like(lax.slice_in_dim(field, 0, 1, axis=axis))
    return jnp.concatenate([edge, rest], axis)

def yee_step(electric, magnetic, keep, curl):
    electric_x, electric_y, electric_z = electric
    magnetic_x, magnetic_y, magnetic_z = magnetic
    magnetic_x = magnetic_x - 0.5 * (shifted_above(electric_z, 1) - electric_z - (shifted_above(electric_y, 2) - electric_y))
    magnetic_y = magnetic_y - 0.5 * (shifted_above(electric_x, 2) - electric_x - (shifted_above(electric_z, 0) - electric_z))
    magnetic_z = magnetic_z - 0.5 * (shifted_above(electric_y, 0) - electric_y - (shifted_above(electric_x, 1) - electric_x))
    electric_x = keep * electric_x + curl * (magnetic_z - shifted_below(magnetic_z, 1) - (magnetic_y - shifted_below(magnetic_y, 2)))
    electric_y = keep * electric_y + curl * (magnetic_x - shifted_below(magnetic_x, 2) - (magnetic_z - shifted_below(magnetic_z, 0)))
    electric_z = keep * electric_z + curl * (magnetic_y - shifted_below(magnetic_y, 0) - (magnetic_x - shifted_below(magnetic_x, 1)))
    return ((electric_x, electric_y, electric_z), (magnetic_x, magnetic_y, magnetic_z))

def split_index(flat):
    first = flat // (NY * NZ)
    second = flat // NZ % NY
    third = flat % NZ
    return (first, second, third)

def reference(permittivity, loss, fwd_electric, fwd_magnetic, adj_electric, adj_magnetic, wavelet, residuals, source_cell, receiver_cells, start_step):
    keep = (1.0 - loss) / (1.0 + loss)
    curl = 0.5 / (permittivity * (1.0 + loss))
    start = start_step[0]
    zero_index = jnp.zeros((), jnp.int32)
    src_i, src_j, src_k = split_index(source_cell[0])
    rec_i, rec_j, rec_k = split_index(receiver_cells)
    electric = (fwd_electric[0], fwd_electric[1], fwd_electric[2])
    magnetic = (fwd_magnetic[0], fwd_magnetic[1], fwd_magnetic[2])
    snapshots = [electric]
    for index in range(STEPS):
        electric, magnetic = yee_step(electric, magnetic, keep, curl)
        sample = lax.dynamic_slice_in_dim(wavelet, start + index, 1)[0]
        electric = (electric[0], electric[1], electric[2].at[src_i, src_j, src_k].add(sample))
        snapshots.append(electric)
    window = lax.dynamic_slice(residuals, (zero_index, start), (residuals.shape[0], STEPS))
    adjoint = (adj_electric[0], adj_electric[1], adj_electric[2])
    adjoint_mag = (adj_magnetic[0], adj_magnetic[1], adj_magnetic[2])
    gradient = jnp.zeros(permittivity.shape, jnp.float32)
    for index in range(STEPS):
        adjoint, adjoint_mag = yee_step(adjoint, adjoint_mag, keep, curl)
        adjoint = (adjoint[0], adjoint[1], adjoint[2].at[rec_i, rec_j, rec_k].add(window[:, STEPS - 1 - index]))
        later = STEPS - index
        change = [snapshots[later][c] - snapshots[later - 1][c] for c in range(3)]
        gradient = gradient + (change[0] * adjoint[0] + change[1] * adjoint[1] + change[2] * adjoint[2])
    gradient = -gradient / permittivity
    grad_rms = jnp.sqrt(jnp.sum(gradient * gradient) / (NX * NY * NZ) + 1e-06)
    return (gradient / grad_rms, grad_rms)
```

```python
import functools

import jax
import jax.numpy as jnp
from jax import lax
from jax.experimental import pallas as pl
from jax.experimental.pallas import tpu as pltpu
from jax.sharding import PartitionSpec as P

STEPS = 4
MESH = pl.DeviceIdType.MESH
F32 = jnp.float32
HALF = 0.5


def kernel(
    sizes,
    wav_ref,
    src_ref,
    start_ref,
    cells_ref,
    perm_hbm,
    loss_hbm,
    fe_hbm,
    fm_hbm,
    ae_hbm,
    am_hbm,
    res_ref,
    out_ref,
    rms_ref,
    E,
    H,
    perm,
    loss,
    keep,
    curl,
    D,
    A,
    inj,
    R,
    grad,
    ysend,
    yrecv,
    zsend,
    zrecv,
    part,
    suma,
    sumb,
    load_sem,
    face_send,
    face_recv,
    ga_send,
    ga_recv,
    gb_send,
    gb_recv,
    ra_send,
    ra_recv,
    rb_send,
    rb_recv,
):
    gx, gy, gz = sizes
    nx, ny, nz = perm.shape
    pad = E.shape[3] - ny
    ix, iy, iz = lax.axis_index("gx"), lax.axis_index("gy"), lax.axis_index("gz")
    nplane = gy * gz
    plane = iy * gz + iz

    loads = [
        pltpu.make_async_copy(fe_hbm, E.at[0, :, 0:nx, 0:ny, :], load_sem.at[0]),
        pltpu.make_async_copy(ae_hbm, E.at[1, :, 0:nx, 0:ny, :], load_sem.at[1]),
        pltpu.make_async_copy(fm_hbm, H.at[0, :, 1 : nx + 1, pad : pad + ny, :], load_sem.at[2]),
        pltpu.make_async_copy(am_hbm, H.at[1, :, 1 : nx + 1, pad : pad + ny, :], load_sem.at[3]),
        pltpu.make_async_copy(loss_hbm, loss, load_sem.at[4]),
        pltpu.make_async_copy(perm_hbm, perm, load_sem.at[5]),
    ]
    for load in loads:
        load.start()

    plane_peers = []
    for d in range(1, nplane):
        q = lax.rem(plane + d, nplane)
        plane_peers.append((q, (ix, q // gz, lax.rem(q, gz))))
    line_peers = []
    for d in range(1, gx):
        q = lax.rem(ix + d, gx)
        line_peers.append((q, (q, iy, iz)))

    zero_plane = jnp.zeros((ny, nz), F32)
    for s in range(2):
        for c in range(3):
            E[s, c, nx, 0:ny, :] = zero_plane
            H[s, c, 0, pad : pad + ny, :] = zero_plane
    yrecv[...] = jnp.zeros(yrecv.shape, F32)
    zrecv[...] = jnp.zeros(zrecv.shape, F32)

    barrier = pltpu.get_barrier_semaphore()
    for _, dev in plane_peers + line_peers:
        pl.semaphore_signal(barrier, inc=1, device_id=dev, device_id_type=MESH)
    pl.semaphore_wait(barrier, len(plane_peers) + len(line_peers))

    def remote(src, dst, ssem, rsem, dev):
        return pltpu.make_async_remote_copy(
            src_ref=src, dst_ref=dst, send_sem=ssem, recv_sem=rsem,
            device_id=dev, device_id_type=MESH,
        )

    per = res_ref.shape[0]

    def rows_of(x, q, count):
        return pl.ds(pl.multiple_of((x * nplane + q) * per, 8), count)

    R[rows_of(ix, plane, per), :] = res_ref[...]
    gather_a = []
    for d, (q, dev) in enumerate(plane_peers):
        send = remote(res_ref, R.at[rows_of(ix, plane, per), :], ga_send.at[d], ga_recv.at[plane], dev)
        recv = remote(res_ref, R.at[rows_of(ix, q, per), :], ga_send.at[d], ga_recv.at[q], dev)
        send.start()
        gather_a.append((send, recv))

    def gather_mid():
        for send, recv in gather_a:
            recv.wait_recv()
        for d, (q, dev) in enumerate(line_peers):
            mine = R.at[rows_of(ix, 0, per * nplane), :]
            remote(mine, mine, gb_send.at[d], gb_recv.at[ix], dev).start()

    def gather_end():
        for d, (q, dev) in enumerate(line_peers):
            theirs = R.at[rows_of(q, 0, per * nplane), :]
            remote(theirs, theirs, gb_send.at[d], gb_recv.at[q], dev).wait()
        for send, recv in gather_a:
            send.wait_send()

    def faces(s, kind):
        low = kind == 0
        step = -1 if low else 1
        field = E if low else H
        rows = slice(0, ny) if low else slice(pad, pad + ny)
        from_x, to_x = (0, nx) if low else (nx, 0)
        idx = (ix, iy, iz)
        size = (gx, gy, gz)
        refs = (
            (field.at[s, 1:3, from_x, rows, :], field.at[s, 1:3, to_x, rows, :]),
            (ysend.at[kind, s], yrecv.at[kind, s]),
            (zsend.at[kind, s], zrecv.at[kind, s]),
        )
        out = []
        for a in range(3):
            if low:
                can_send, can_recv = idx[a] > 0, idx[a] < size[a] - 1
            else:
                can_send, can_recv = idx[a] < size[a] - 1, idx[a] > 0
            dev = [ix, iy, iz]
            dev[a] = jnp.clip(idx[a] + step, 0, size[a] - 1)
            copy = remote(refs[a][0], refs[a][1], face_send.at[kind, s, a], face_recv.at[kind, s, a], tuple(dev))
            out.append((copy, can_send, can_recv))
        return out

    def start(face, extra=None):
        copy, can_send, _ = face
        cond = can_send if extra is None else can_send & extra

        @pl.when(cond)
        def _():
            copy.start()

    def finish(face):
        copy, can_send, _ = face

        @pl.when(can_send)
        def _():
            copy.wait_send()

    def arrive(face):
        copy, _, can_recv = face

        @pl.when(can_recv)
        def _():
            copy.wait_recv()

    lane = lax.broadcasted_iota(jnp.int32, (ny, nz), 1)
    row = lax.broadcasted_iota(jnp.int32, (ny, nz), 0)

    def pack_column(acc, value, source, j):
        return jnp.where(lane == j, pltpu.roll(value, (j - source) % nz, 1), acc)

    def up_z(value, halo, j):
        return jnp.where(lane == nz - 1, pltpu.roll(halo, (nz - 1 - j) % nz, 1), pltpu.roll(value, nz - 1, 1))

    def down_z(value, halo, j):
        rolled = pltpu.roll(value, 1, 1)
        return jnp.where(lane == 0, pltpu.roll(halo, (nz - j) % nz, 1), rolled)

    def send_first(s):
        acc = jnp.zeros((ny, nz), F32)
        face = faces(s, 0)
        start(face[0])
        for p in range(nx):
            ysend[0, s, 0, p : p + 1, :] = E[s, 0, p, 0:1, :]
            ysend[0, s, 1, p : p + 1, :] = E[s, 2, p, 0:1, :]
            acc = pack_column(acc, E[s, 0, p, 0:ny, :], 0, p)
            acc = pack_column(acc, E[s, 1, p, 0:ny, :], 0, nx + p)
        zsend[0, s] = acc
        start(face[1])
        start(face[2])

    def update_h(s):
        came = faces(s, 0)
        going = faces(s, 1)
        for face in came:
            arrive(face)
        for p in range(nx):
            E[s, 0, p, ny : ny + 1, :] = yrecv[0, s, 0, p : p + 1, :]
            E[s, 2, p, ny : ny + 1, :] = yrecv[0, s, 1, p : p + 1, :]
        halo = zrecv[0, s]
        acc = jnp.zeros((ny, nz), F32)
        inner = slice(pad, pad + ny)
        for p in reversed(range(nx)):
            ex, ey, ez = E[s, 0, p, 0:ny, :], E[s, 1, p, 0:ny, :], E[s, 2, p, 0:ny, :]
            hx = H[s, 0, p + 1, inner, :] - HALF * (E[s, 2, p, 1 : ny + 1, :] - ez - (up_z(ey, halo, nx + p) - ey))
            hy = H[s, 1, p + 1, inner, :] - HALF * (up_z(ex, halo, p) - ex - (E[s, 2, p + 1, 0:ny, :] - ez))
            hz = H[s, 2, p + 1, inner, :] - HALF * (E[s, 1, p + 1, 0:ny, :] - ey - (E[s, 0, p, 1 : ny + 1, :] - ex))
            H[s, 0, p + 1, inner, :] = hx
            H[s, 1, p + 1, inner, :] = hy
            H[s, 2, p + 1, inner, :] = hz
            if p == nx - 1:
                start(going[0])
            ysend[1, s, 0, p : p + 1, :] = hx[ny - 1 : ny, :]
            ysend[1, s, 1, p : p + 1, :] = hz[ny - 1 : ny, :]
            acc = pack_column(acc, hx, nz - 1, p)
            acc = pack_column(acc, hy, nz - 1, nx + p)
        zsend[1, s] = acc
        start(going[1])
        start(going[2])

    src = src_ref[0]
    begin = start_ref[0]
    total_z, total_y = nz * gz, ny * gy
    src_i = lax.div(src, total_y * total_z) - ix * nx
    src_j = lax.rem(lax.div(src, total_z), total_y) - iy * ny
    src_k = lax.rem(src, total_z) - iz * nz
    src_mask = (row == src_j) & (lane == src_k)

    def update_e(s, k):
        came = faces(s, 1)
        going = faces(s, 0)
        for face in came:
            arrive(face)
        for face in going:
            finish(face)
        for p in range(nx):
            H[s, 0, p + 1, pad - 1 : pad, :] = yrecv[1, s, 0, p : p + 1, :]
            H[s, 2, p + 1, pad - 1 : pad, :] = yrecv[1, s, 1, p : p + 1, :]
        more = k < STEPS - 1
        halo = zrecv[1, s]
        acc = jnp.zeros((ny, nz), F32)
        inner = slice(pad, pad + ny)
        below = slice(pad - 1, pad + ny - 1)
        pulse = wav_ref[begin + k]
        for p in range(nx):
            hx, hy, hz = H[s, 0, p + 1, inner, :], H[s, 1, p + 1, inner, :], H[s, 2, p + 1, inner, :]
            kp, cl = keep[p], curl[p]
            ox, oy, oz = E[s, 0, p, 0:ny, :], E[s, 1, p, 0:ny, :], E[s, 2, p, 0:ny, :]
            ex = kp * ox + cl * (hz - H[s, 2, p + 1, below, :] - (hy - down_z(hy, halo, nx + p)))
            ey = kp * oy + cl * (hx - down_z(hx, halo, p) - (hz - H[s, 2, p, inner, :]))
            ez = kp * oz + cl * (hy - H[s, 1, p, inner, :] - (hx - H[s, 0, p + 1, below, :]))
            if s == 0:
                ez = ez + jnp.where(src_mask, jnp.where(src_i == p, pulse, 0.0), 0.0)
                D[k, 0, p] = ex - ox
                D[k, 1, p] = ey - oy
                D[k, 2, p] = ez - oz
            else:
                ez = ez + inj[k, p * ny : (p + 1) * ny, :]
                A[k, 0, p] = ex
                A[k, 1, p] = ey
                A[k, 2, p] = ez
            E[s, 0, p, 0:ny, :] = ex
            E[s, 1, p, 0:ny, :] = ey
            E[s, 2, p, 0:ny, :] = ez
            if p == 0:
                start(going[0], more)
            ysend[0, s, 0, p : p + 1, :] = ex[0:1, :]
            ysend[0, s, 1, p : p + 1, :] = ez[0:1, :]
            acc = pack_column(acc, ex, 0, p)
            acc = pack_column(acc, ey, 0, nx + p)
        zsend[0, s] = acc
        start(going[1], more)
        start(going[2], more)
        for face in came_out(s):
            finish(face)

    def came_out(s):
        return faces(s, 1)

    def injection():
        cells = cells_ref[...]
        count = cells.shape[1]
        i = lax.div(cells, total_y * total_z) - ix * nx
        j = lax.rem(lax.div(cells, total_z), total_y) - iy * ny
        k = lax.rem(cells, total_z) - iz * nz
        inside = (i >= 0) & (i < nx) & (j >= 0) & (j < ny)
        where = jnp.where(inside, i * ny + j, -1)
        rows = lax.broadcasted_iota(jnp.int32, (nx * ny, count), 0)
        spots = jnp.where(rows == where, 1.0, 0.0).astype(jnp.bfloat16)
        depth = lax.broadcasted_iota(jnp.int32, (nz, count), 0) == k
        trace = R.shape[1]
        pick_lane = lax.broadcasted_iota(jnp.int32, (8, trace), 1)
        pick_row = lax.broadcasted_iota(jnp.int32, (8, trace), 0)
        pick = jnp.where(pick_lane == begin + STEPS - 1 - pick_row, 1.0, 0.0)
        nt = (((1,), (1,)), ((), ()))
        samples = lax.dot_general(pick, R[...], nt, precision=lax.Precision.HIGHEST, preferred_element_type=F32)
        for m in range(STEPS):
            rest = jnp.where(depth, samples[m : m + 1, :], 0.0)
            total = jnp.zeros((nx * ny, nz), F32)
            for _ in range(3):
                head = rest.astype(jnp.bfloat16)
                rest = rest - head.astype(F32)
                total = total + lax.dot_general(spots, head, nt, preferred_element_type=F32)
            inj[m] = total

    loads[0].wait()
    send_first(0)
    loads[1].wait()
    send_first(1)
    loads[4].wait()
    loads[5].wait()
    for p in range(nx):
        lo = loss[p]
        keep[p] = (1.0 - lo) / (1.0 + lo)
        curl[p] = 0.5 / (perm[p] * (1.0 + lo))
    loads[2].wait()
    loads[3].wait()

    update_h(0)
    gather_mid()
    update_h(1)
    update_e(0, 0)
    gather_end()
    injection()
    update_e(1, 0)

    def body(k, carry):
        update_h(0)
        update_h(1)
        update_e(0, k)
        update_e(1, k)
        return carry

    lax.fori_loop(1, STEPS, body, 0)

    squares = jnp.zeros((ny, nz), F32)
    for p in range(nx):
        total = jnp.zeros((ny, nz), F32)
        for m in range(STEPS):
            n = STEPS - 1 - m
            total = total + (D[n, 0, p] * A[m, 0, p] + D[n, 1, p] * A[m, 1, p] + D[n, 2, p] * A[m, 2, p])
        g = -total / perm[p]
        grad[p] = g
        squares = squares + g * g
    tile = squares[0:8, :]
    for r in range(1, ny // 8):
        tile = tile + squares[8 * r : 8 * r + 8, :]
    part[0] = tile

    def reduce(src, slots, me, peers, send_sems, recv_sems, count):
        slots[pl.ds(me, 1)] = src[...][None]
        copies = []
        for d, (q, dev) in enumerate(peers):
            send = remote(src, slots.at[me], send_sems.at[d], recv_sems.at[me], dev)
            recv = remote(src, slots.at[q], send_sems.at[d], recv_sems.at[q], dev)
            send.start()
            copies.append((send, recv))
        for send, recv in copies:
            recv.wait_recv()
        out = slots[0]
        for q in range(1, count):
            out = out + slots[q]
        for send, recv in copies:
            send.wait_send()
        return out

    part[1] = reduce(part.at[0], suma, plane, plane_peers, ra_send, ra_recv, nplane)
    tile = reduce(part.at[1], sumb, ix, line_peers, rb_send, rb_recv, gx)
    total = jnp.sum(jnp.sum(tile, axis=0, keepdims=True), axis=1, keepdims=True)
    rms = jnp.sqrt(total / (nx * ny * nz * gx * gy * gz) + 1e-06)
    rms_ref[...] = rms
    inverse = 1.0 / rms
    for p in range(nx):
        out_ref[p] = grad[p] * inverse


def per_device(
    permittivity, loss, fwd_electric, fwd_magnetic, adj_electric, adj_magnetic,
    wavelet, residuals, source_cell, receiver_cells, start_step,
):
    sizes = tuple(lax.axis_size(a) for a in ("gx", "gy", "gz"))
    gx, gy, gz = sizes
    nx, ny, nz = permittivity.shape
    nplane = gy * gz
    count = receiver_cells.shape[0]
    trace = residuals.shape[1]
    smem = pl.BlockSpec(memory_space=pltpu.SMEM)
    vmem = pl.BlockSpec(memory_space=pltpu.VMEM)
    hbm = pl.BlockSpec(memory_space=pl.ANY)
    dma = pltpu.SemaphoreType.DMA
    block = (nx, ny, nz)
    padded = (2, 3, nx + 1, ny + 8, nz)
    direction, rms = pl.pallas_call(
        functools.partial(kernel, sizes),
        out_shape=(
            jax.ShapeDtypeStruct(block, F32),
            jax.ShapeDtypeStruct((1, 1), F32),
        ),
        in_specs=[smem, smem, smem, vmem, hbm, hbm, hbm, hbm, hbm, hbm, vmem],
        out_specs=(vmem, vmem),
        scratch_shapes=[
            pltpu.VMEM(padded, F32),
            pltpu.VMEM(padded, F32),
            pltpu.VMEM(block, F32),
            pltpu.VMEM(block, F32),
            pltpu.VMEM(block, F32),
            pltpu.VMEM(block, F32),
            pltpu.VMEM((STEPS, 3) + block, F32),
            pltpu.VMEM((STEPS, 3) + block, F32),
            pltpu.VMEM((STEPS, nx * ny, nz), F32),
            pltpu.VMEM((count, trace), F32),
            pltpu.VMEM(block, F32),
            pltpu.VMEM((2, 2, 2, nx, nz), F32),
            pltpu.VMEM((2, 2, 2, nx, nz), F32),
            pltpu.VMEM((2, 2, ny, nz), F32),
            pltpu.VMEM((2, 2, ny, nz), F32),
            pltpu.VMEM((2, 8, nz), F32),
            pltpu.VMEM((nplane, 8, nz), F32),
            pltpu.VMEM((gx, 8, nz), F32),
            dma((6,)),
            dma((2, 2, 3)),
            dma((2, 2, 3)),
            dma((nplane,)),
            dma((nplane,)),
            dma((gx,)),
            dma((gx,)),
            dma((nplane,)),
            dma((nplane,)),
            dma((gx,)),
            dma((gx,)),
        ],
        compiler_params=pltpu.CompilerParams(
            collective_id=0, has_side_effects=True, vmem_limit_bytes=60 * 1024 * 1024
        ),
    )(
        wavelet, source_cell, start_step, receiver_cells.reshape(1, count),
        permittivity, loss, fwd_electric, fwd_magnetic, adj_electric, adj_magnetic, residuals,
    )
    return direction, rms.reshape(())


def solution(mesh):
    block = P("gx", "gy", "gz")
    state = P(None, "gx", "gy", "gz")
    return jax.shard_map(
        per_device,
        mesh=mesh,
        in_specs=(
            block, block, state, state, state, state,
            P(), P(("gx", "gy", "gz"), None), P(), P(), P(),
        ),
        out_specs=(block, P()),
        check_vma=False,
    )
```

```python
import functools

import jax
import jax.numpy as jnp
from jax import lax
from jax.experimental import pallas as pl
from jax.experimental.pallas import tpu as pltpu
from jax.sharding import PartitionSpec as P

STEPS = 4
MESH = pl.DeviceIdType.MESH
F32 = jnp.float32
HALF = 0.5


def kernel(
    sizes,
    wav_hbm,
    src_hbm,
    start_hbm,
    cells_hbm,
    perm_hbm,
    loss_hbm,
    fe_hbm,
    fm_hbm,
    ae_hbm,
    am_hbm,
    res_hbm,
    out_ref,
    rms_ref,
    E,
    H,
    perm,
    loss,
    keep,
    curl,
    D,
    A,
    inj,
    R,
    grad,
    ysend,
    yrecv,
    zsend,
    zrecv,
    part,
    sums,
    wav_ref,
    src_ref,
    start_ref,
    cells_ref,
    res_ref,
    mine,
    load_sem,
    face_send,
    face_recv,
    g_send,
    g_recv,
    r_send,
    r_recv,
):
    gx, gy, gz = sizes
    nx, ny, nz = perm.shape
    pad = E.shape[3] - ny
    ix, iy, iz = lax.axis_index("gx"), lax.axis_index("gy"), lax.axis_index("gz")
    nplane = gy * gz
    plane = iy * gz + iz

    loads = [
        pltpu.make_async_copy(fe_hbm, E.at[0, :, 0:nx, 0:ny, :], load_sem.at[0]),
        pltpu.make_async_copy(ae_hbm, E.at[1, :, 0:nx, 0:ny, :], load_sem.at[1]),
        pltpu.make_async_copy(fm_hbm, H.at[0, :, 1 : nx + 1, pad : pad + ny, :], load_sem.at[2]),
        pltpu.make_async_copy(am_hbm, H.at[1, :, 1 : nx + 1, pad : pad + ny, :], load_sem.at[3]),
        pltpu.make_async_copy(loss_hbm, loss, load_sem.at[4]),
        pltpu.make_async_copy(perm_hbm, perm, load_sem.at[5]),
    ]
    small = [
        pltpu.make_async_copy(start_hbm, start_ref, load_sem.at[6]),
        pltpu.make_async_copy(res_hbm, res_ref, load_sem.at[7]),
        pltpu.make_async_copy(src_hbm, src_ref, load_sem.at[8]),
        pltpu.make_async_copy(wav_hbm, wav_ref, load_sem.at[9]),
        pltpu.make_async_copy(cells_hbm, cells_ref, load_sem.at[10]),
    ]
    loads = loads + small
    for load in small:
        load.start()
    loads, small = loads[:6], loads[6:]
    for load in loads:
        load.start()

    total_devices = gx * nplane
    me = ix * nplane + plane
    peers = []
    for d in range(1, total_devices):
        q = lax.rem(me + d, total_devices)
        peers.append((q, (q // nplane, lax.rem(q // gz, gy), lax.rem(q, gz))))

    zero_plane = jnp.zeros((ny, nz), F32)
    for s in range(2):
        for c in range(3):
            E[s, c, nx, 0:ny, :] = zero_plane
            H[s, c, 0, pad : pad + ny, :] = zero_plane
    yrecv[...] = jnp.zeros(yrecv.shape, F32)
    zrecv[...] = jnp.zeros(zrecv.shape, F32)

    barrier = pltpu.get_barrier_semaphore()
    for _, dev in peers:
        pl.semaphore_signal(barrier, inc=1, device_id=dev, device_id_type=MESH)

    per, trace = res_hbm.shape
    small[0].wait()
    small[1].wait()
    begin = start_ref[0]
    time_at = lax.broadcasted_iota(jnp.int32, (trace, nz), 0)
    slot = lax.div(lax.broadcasted_iota(jnp.int32, (trace, nz), 1), per)
    pick = jnp.where(time_at == begin + STEPS - 1 - slot, 1.0, 0.0)
    wide = jnp.dot(res_ref[...], pick, precision=lax.Precision.HIGHEST, preferred_element_type=F32)
    own = lax.rem(lax.broadcasted_iota(jnp.int32, (per, nz), 1), per)
    own = own == lax.broadcasted_iota(jnp.int32, (per, nz), 0)
    mine[0] = jnp.sum(jnp.where(own, wide, 0.0), axis=0, keepdims=True)
    R[pl.ds(me, 1)] = mine[...]
    for load in small[2:]:
        load.wait()
    pl.semaphore_wait(barrier, len(peers))

    def remote(src, dst, ssem, rsem, dev):
        return pltpu.make_async_remote_copy(
            src_ref=src, dst_ref=dst, send_sem=ssem, recv_sem=rsem,
            device_id=dev, device_id_type=MESH,
        )

    def exchange(src, slots, send_sems, recv_sems):
        copies = []
        for d, (q, dev) in enumerate(peers):
            send = remote(src, slots.at[me], send_sems.at[d], recv_sems.at[me], dev)
            recv = remote(src, slots.at[q], send_sems.at[d], recv_sems.at[q], dev)
            send.start()
            copies.append((send, recv))
        return copies

    def settle(copies):
        for send, recv in copies:
            recv.wait_recv()
        for send, recv in copies:
            send.wait_send()

    def faces(s, kind):
        low = kind == 0
        step = -1 if low else 1
        field = E if low else H
        rows = slice(0, ny) if low else slice(pad, pad + ny)
        from_x, to_x = (0, nx) if low else (nx, 0)
        idx = (ix, iy, iz)
        size = (gx, gy, gz)
        refs = (
            (field.at[s, 1:3, from_x, rows, :], field.at[s, 1:3, to_x, rows, :]),
            (ysend.at[kind, s], yrecv.at[kind, s]),
            (zsend.at[kind, s], zrecv.at[kind, s]),
        )
        out = []
        for a in range(3):
            if low:
                can_send, can_recv = idx[a] > 0, idx[a] < size[a] - 1
            else:
                can_send, can_recv = idx[a] < size[a] - 1, idx[a] > 0
            dev = [ix, iy, iz]
            dev[a] = jnp.clip(idx[a] + step, 0, size[a] - 1)
            copy = remote(refs[a][0], refs[a][1], face_send.at[kind, s, a], face_recv.at[kind, s, a], tuple(dev))
            out.append((copy, can_send, can_recv))
        return out

    def start(face, extra=None):
        copy, can_send, _ = face
        cond = can_send if extra is None else can_send & extra

        @pl.when(cond)
        def _():
            copy.start()

    def finish(face):
        copy, can_send, _ = face

        @pl.when(can_send)
        def _():
            copy.wait_send()

    def arrive(face):
        copy, _, can_recv = face

        @pl.when(can_recv)
        def _():
            copy.wait_recv()

    lane = lax.broadcasted_iota(jnp.int32, (ny, nz), 1)
    row = lax.broadcasted_iota(jnp.int32, (ny, nz), 0)

    def pack_column(acc, value, source, j):
        return jnp.where(lane == j, pltpu.roll(value, (j - source) % nz, 1), acc)

    def up_z(value, halo, j):
        return jnp.where(lane == nz - 1, pltpu.roll(halo, (nz - 1 - j) % nz, 1), pltpu.roll(value, nz - 1, 1))

    def down_z(value, halo, j):
        rolled = pltpu.roll(value, 1, 1)
        return jnp.where(lane == 0, pltpu.roll(halo, (nz - j) % nz, 1), rolled)

    def send_first(s):
        acc = jnp.zeros((ny, nz), F32)
        face = faces(s, 0)
        start(face[0])
        for p in range(nx):
            ysend[0, s, 0, p : p + 1, :] = E[s, 0, p, 0:1, :]
            ysend[0, s, 1, p : p + 1, :] = E[s, 2, p, 0:1, :]
            acc = pack_column(acc, E[s, 0, p, 0:ny, :], 0, p)
            acc = pack_column(acc, E[s, 1, p, 0:ny, :], 0, nx + p)
        zsend[0, s] = acc
        start(face[1])
        start(face[2])

    def update_h(s):
        came = faces(s, 0)
        going = faces(s, 1)
        for face in came:
            arrive(face)
        for p in range(nx):
            E[s, 0, p, ny : ny + 1, :] = yrecv[0, s, 0, p : p + 1, :]
            E[s, 2, p, ny : ny + 1, :] = yrecv[0, s, 1, p : p + 1, :]
        halo = zrecv[0, s]
        acc = jnp.zeros((ny, nz), F32)
        inner = slice(pad, pad + ny)
        for p in reversed(range(nx)):
            ex, ey, ez = E[s, 0, p, 0:ny, :], E[s, 1, p, 0:ny, :], E[s, 2, p, 0:ny, :]
            hx = H[s, 0, p + 1, inner, :] - HALF * (E[s, 2, p, 1 : ny + 1, :] - ez - (up_z(ey, halo, nx + p) - ey))
            hy = H[s, 1, p + 1, inner, :] - HALF * (up_z(ex, halo, p) - ex - (E[s, 2, p + 1, 0:ny, :] - ez))
            hz = H[s, 2, p + 1, inner, :] - HALF * (E[s, 1, p + 1, 0:ny, :] - ey - (E[s, 0, p, 1 : ny + 1, :] - ex))
            H[s, 0, p + 1, inner, :] = hx
            H[s, 1, p + 1, inner, :] = hy
            H[s, 2, p + 1, inner, :] = hz
            if p == nx - 1:
                start(going[0])
            ysend[1, s, 0, p : p + 1, :] = hx[ny - 1 : ny, :]
            ysend[1, s, 1, p : p + 1, :] = hz[ny - 1 : ny, :]
            acc = pack_column(acc, hx, nz - 1, p)
            acc = pack_column(acc, hy, nz - 1, nx + p)
        zsend[1, s] = acc
        start(going[1])
        start(going[2])

    src = src_ref[0]
    total_z, total_y = nz * gz, ny * gy
    src_i = lax.div(src, total_y * total_z) - ix * nx
    src_j = lax.rem(lax.div(src, total_z), total_y) - iy * ny
    src_k = lax.rem(src, total_z) - iz * nz
    src_mask = (row == src_j) & (lane == src_k)

    def update_e(s, k):
        came = faces(s, 1)
        going = faces(s, 0)
        for face in came:
            arrive(face)
        for face in going:
            finish(face)
        for p in range(nx):
            H[s, 0, p + 1, pad - 1 : pad, :] = yrecv[1, s, 0, p : p + 1, :]
            H[s, 2, p + 1, pad - 1 : pad, :] = yrecv[1, s, 1, p : p + 1, :]
        more = k < STEPS - 1
        halo = zrecv[1, s]
        acc = jnp.zeros((ny, nz), F32)
        inner = slice(pad, pad + ny)
        below = slice(pad - 1, pad + ny - 1)
        pulse = wav_ref[begin + k]
        for p in range(nx):
            hx, hy, hz = H[s, 0, p + 1, inner, :], H[s, 1, p + 1, inner, :], H[s, 2, p + 1, inner, :]
            kp, cl = keep[p], curl[p]
            ox, oy, oz = E[s, 0, p, 0:ny, :], E[s, 1, p, 0:ny, :], E[s, 2, p, 0:ny, :]
            ex = kp * ox + cl * (hz - H[s, 2, p + 1, below, :] - (hy - down_z(hy, halo, nx + p)))
            ey = kp * oy + cl * (hx - down_z(hx, halo, p) - (hz - H[s, 2, p, inner, :]))
            ez = kp * oz + cl * (hy - H[s, 1, p, inner, :] - (hx - H[s, 0, p + 1, below, :]))
            if s == 0:
                ez = ez + jnp.where(src_mask, jnp.where(src_i == p, pulse, 0.0), 0.0)
                D[k, 0, p] = ex - ox
                D[k, 1, p] = ey - oy
                D[k, 2, p] = ez - oz
            else:
                ez = ez + inj[k, p * ny : (p + 1) * ny, :]
                A[k, 0, p] = ex
                A[k, 1, p] = ey
                A[k, 2, p] = ez
            E[s, 0, p, 0:ny, :] = ex
            E[s, 1, p, 0:ny, :] = ey
            E[s, 2, p, 0:ny, :] = ez
            if p == 0:
                start(going[0], more)
            ysend[0, s, 0, p : p + 1, :] = ex[0:1, :]
            ysend[0, s, 1, p : p + 1, :] = ez[0:1, :]
            acc = pack_column(acc, ex, 0, p)
            acc = pack_column(acc, ey, 0, nx + p)
        zsend[0, s] = acc
        start(going[1], more)
        start(going[2], more)
        for face in came_out(s):
            finish(face)

    def came_out(s):
        return faces(s, 1)

    def injection():
        cells = cells_ref[...]
        count = cells.shape[1]
        i = lax.div(cells, total_y * total_z) - ix * nx
        j = lax.rem(lax.div(cells, total_z), total_y) - iy * ny
        k = lax.rem(cells, total_z) - iz * nz
        inside = (i >= 0) & (i < nx) & (j >= 0) & (j < ny)
        where = jnp.where(inside, i * ny + j, -1)
        rows = lax.broadcasted_iota(jnp.int32, (nx * ny, count), 0)
        spots = jnp.where(rows == where, 1.0, 0.0).astype(jnp.bfloat16)
        depth = lax.broadcasted_iota(jnp.int32, (nz, count), 0) == k
        nt = (((1,), (1,)), ((), ()))
        spread_lane = lax.broadcasted_iota(jnp.int32, (nz, count), 0)
        spread_rec = lax.rem(lax.broadcasted_iota(jnp.int32, (nz, count), 1), per)
        holder = lax.div(lax.broadcasted_iota(jnp.int32, (total_devices, count), 1), per)
        holder = holder == lax.broadcasted_iota(jnp.int32, (total_devices, count), 0)
        packed = R[:, 0, :]
        for m in range(STEPS):
            spread = jnp.where(spread_lane == m * per + spread_rec, 1.0, 0.0)
            found = jnp.dot(packed, spread, precision=lax.Precision.HIGHEST, preferred_element_type=F32)
            samples = jnp.sum(jnp.where(holder, found, 0.0), axis=0, keepdims=True)
            rest = jnp.where(depth, samples, 0.0)
            total = jnp.zeros((nx * ny, nz), F32)
            for _ in range(3):
                head = rest.astype(jnp.bfloat16)
                rest = rest - head.astype(F32)
                total = total + lax.dot_general(spots, head, nt, preferred_element_type=F32)
            inj[m] = total

    loads[0].wait()
    send_first(0)
    loads[1].wait()
    send_first(1)
    gather = exchange(mine.at[0], R, g_send, g_recv)
    loads[4].wait()
    loads[5].wait()
    for p in range(nx):
        lo = loss[p]
        keep[p] = (1.0 - lo) / (1.0 + lo)
        curl[p] = 0.5 / (perm[p] * (1.0 + lo))
    loads[2].wait()
    loads[3].wait()

    update_h(0)
    update_h(1)
    update_e(0, 0)
    settle(gather)
    injection()
    update_e(1, 0)

    def body(k, carry):
        update_h(0)
        update_h(1)
        update_e(0, k)
        update_e(1, k)
        return carry

    lax.fori_loop(1, STEPS, body, 0)

    squares = jnp.zeros((ny, nz), F32)
    for p in range(nx):
        total = jnp.zeros((ny, nz), F32)
        for m in range(STEPS):
            n = STEPS - 1 - m
            total = total + (D[n, 0, p] * A[m, 0, p] + D[n, 1, p] * A[m, 1, p] + D[n, 2, p] * A[m, 2, p])
        g = -total / perm[p]
        grad[p] = g
        squares = squares + g * g
    part[0] = jnp.sum(squares, axis=0, keepdims=True)
    sums[pl.ds(me, 1)] = part[...]
    settle(exchange(part.at[0], sums, r_send, r_recv))
    tile = sums[:, 0, :]
    total = jnp.sum(jnp.sum(tile, axis=0, keepdims=True), axis=1, keepdims=True)
    rms = jnp.sqrt(total / (nx * ny * nz * gx * gy * gz) + 1e-06)
    rms_ref[...] = rms
    inverse = 1.0 / rms
    for p in range(nx):
        out_ref[p] = grad[p] * inverse


def per_device(
    permittivity, loss, fwd_electric, fwd_magnetic, adj_electric, adj_magnetic,
    wavelet, residuals, source_cell, receiver_cells, start_step,
):
    sizes = tuple(lax.axis_size(a) for a in ("gx", "gy", "gz"))
    gx, gy, gz = sizes
    nx, ny, nz = permittivity.shape
    devices = gx * gy * gz
    count = receiver_cells.shape[0]
    vmem = pl.BlockSpec(memory_space=pltpu.VMEM)
    hbm = pl.BlockSpec(memory_space=pltpu.HBM)
    dma = pltpu.SemaphoreType.DMA
    block = (nx, ny, nz)
    padded = (2, 3, nx + 1, ny + 8, nz)
    direction, rms = pl.pallas_call(
        functools.partial(kernel, sizes),
        out_shape=(
            pltpu.VMEM(block, F32),
            jax.ShapeDtypeStruct((1, 1), F32),
        ),
        in_specs=[hbm] * 11,
        out_specs=(vmem, vmem),
        scratch_shapes=[
            pltpu.VMEM(padded, F32),
            pltpu.VMEM(padded, F32),
            pltpu.VMEM(block, F32),
            pltpu.VMEM(block, F32),
            pltpu.VMEM(block, F32),
            pltpu.VMEM(block, F32),
            pltpu.VMEM((STEPS, 3) + block, F32),
            pltpu.VMEM((STEPS, 3) + block, F32),
            pltpu.VMEM((STEPS, nx * ny, nz), F32),
            pltpu.VMEM((devices, 1, nz), F32),
            pltpu.VMEM(block, F32),
            pltpu.VMEM((2, 2, 2, nx, nz), F32),
            pltpu.VMEM((2, 2, 2, nx, nz), F32),
            pltpu.VMEM((2, 2, ny, nz), F32),
            pltpu.VMEM((2, 2, ny, nz), F32),
            pltpu.VMEM((1, 1, nz), F32),
            pltpu.VMEM((devices, 1, nz), F32),
            pltpu.SMEM(wavelet.shape, F32),
            pltpu.SMEM((1,), jnp.int32),
            pltpu.SMEM((1,), jnp.int32),
            pltpu.VMEM((1, count), jnp.int32),
            pltpu.VMEM(residuals.shape, F32),
            pltpu.VMEM((1, 1, nz), F32),
            dma((11,)),
            dma((2, 2, 3)),
            dma((2, 2, 3)),
            dma((devices,)),
            dma((devices,)),
            dma((devices,)),
            dma((devices,)),
        ],
        compiler_params=pltpu.CompilerParams(
            collective_id=0, has_side_effects=True, vmem_limit_bytes=60 * 1024 * 1024
        ),
    )(
        wavelet, source_cell, start_step, receiver_cells.reshape(1, count),
        permittivity, loss, fwd_electric, fwd_magnetic, adj_electric, adj_magnetic, residuals,
    )
    return direction, rms.reshape(())


def solution(mesh):
    block = P("gx", "gy", "gz")
    state = P(None, "gx", "gy", "gz")
    return jax.shard_map(
        per_device,
        mesh=mesh,
        in_specs=(
            block, block, state, state, state, state,
            P(), P(("gx", "gy", "gz"), None), P(), P(), P(),
        ),
        out_specs=(block, P()),
        check_vma=False,
    )
```

```python
import functools

import jax
import jax.numpy as jnp
from jax import lax
from jax.experimental import pallas as pl
from jax.experimental.pallas import tpu as pltpu
from jax.sharding import PartitionSpec as P

STEPS = 4
MESH = pl.DeviceIdType.MESH
F32 = jnp.float32
HALF = 0.5


def kernel(
    sizes,
    wav_hbm,
    src_hbm,
    start_hbm,
    cells_hbm,
    perm_hbm,
    loss_hbm,
    fe_hbm,
    fm_hbm,
    ae_hbm,
    am_hbm,
    res_hbm,
    out_ref,
    rms_ref,
    E,
    H,
    perm,
    loss,
    keep,
    curl,
    D,
    A,
    inj,
    R,
    grad,
    ysend,
    yrecv,
    zsend,
    zrecv,
    part,
    sums,
    wav_ref,
    src_ref,
    start_ref,
    cells_ref,
    res_ref,
    mine,
    load_sem,
    face_send,
    face_recv,
    g_send,
    g_recv,
    r_send,
    r_recv,
):
    gx, gy, gz = sizes
    nx, ny, nz = perm.shape
    pad = E.shape[3] - ny
    ix, iy, iz = lax.axis_index("gx"), lax.axis_index("gy"), lax.axis_index("gz")
    nplane = gy * gz
    plane = iy * gz + iz

    loads = [
        pltpu.make_async_copy(fe_hbm, E.at[0, :, 0:nx, 0:ny, :], load_sem.at[0]),
        pltpu.make_async_copy(ae_hbm, E.at[1, :, 0:nx, 0:ny, :], load_sem.at[1]),
        pltpu.make_async_copy(fm_hbm, H.at[0, :, 1 : nx + 1, pad : pad + ny, :], load_sem.at[2]),
        pltpu.make_async_copy(am_hbm, H.at[1, :, 1 : nx + 1, pad : pad + ny, :], load_sem.at[3]),
        pltpu.make_async_copy(loss_hbm, loss, load_sem.at[4]),
        pltpu.make_async_copy(perm_hbm, perm, load_sem.at[5]),
    ]
    small = [
        pltpu.make_async_copy(start_hbm, start_ref, load_sem.at[6]),
        pltpu.make_async_copy(res_hbm, res_ref, load_sem.at[7]),
        pltpu.make_async_copy(src_hbm, src_ref, load_sem.at[8]),
        pltpu.make_async_copy(wav_hbm, wav_ref, load_sem.at[9]),
        pltpu.make_async_copy(cells_hbm, cells_ref, load_sem.at[10]),
    ]
    loads = loads + small
    for load in small:
        load.start()
    loads, small = loads[:6], loads[6:]
    for load in loads:
        load.start()

    total_devices = gx * nplane
    me = ix * nplane + plane
    peers = []
    for d in range(1, total_devices):
        q = lax.rem(me + d, total_devices)
        peers.append((q, (q // nplane, lax.rem(q // gz, gy), lax.rem(q, gz))))

    zero_plane = jnp.zeros((ny, nz), F32)
    for s in range(2):
        for c in range(3):
            E[s, c, nx, 0:ny, :] = zero_plane
            H[s, c, 0, pad : pad + ny, :] = zero_plane
    yrecv[...] = jnp.zeros(yrecv.shape, F32)
    zrecv[...] = jnp.zeros(zrecv.shape, F32)

    barrier = pltpu.get_barrier_semaphore()
    for _, dev in peers:
        pl.semaphore_signal(barrier, inc=1, device_id=dev, device_id_type=MESH)

    per, trace = res_hbm.shape
    small[0].wait()
    small[1].wait()
    begin = start_ref[0]
    time_at = lax.broadcasted_iota(jnp.int32, (trace, nz), 0)
    slot = lax.div(lax.broadcasted_iota(jnp.int32, (trace, nz), 1), per)
    pick = jnp.where(time_at == begin + STEPS - 1 - slot, 1.0, 0.0)
    wide = jnp.dot(res_ref[...], pick, precision=lax.Precision.HIGHEST, preferred_element_type=F32)
    own = lax.rem(lax.broadcasted_iota(jnp.int32, (per, nz), 1), per)
    own = own == lax.broadcasted_iota(jnp.int32, (per, nz), 0)
    mine[0] = jnp.sum(jnp.where(own, wide, 0.0), axis=0, keepdims=True)
    R[pl.ds(me, 1)] = mine[...]
    for load in small[2:]:
        load.wait()
    pl.semaphore_wait(barrier, len(peers))

    def remote(src, dst, ssem, rsem, dev):
        return pltpu.make_async_remote_copy(
            src_ref=src, dst_ref=dst, send_sem=ssem, recv_sem=rsem,
            device_id=dev, device_id_type=MESH,
        )

    def exchange(src, slots, send_sems, recv_sems):
        copies = []
        for d, (q, dev) in enumerate(peers):
            send = remote(src, slots.at[me], send_sems.at[d], recv_sems.at[me], dev)
            recv = remote(src, slots.at[q], send_sems.at[d], recv_sems.at[q], dev)
            send.start()
            copies.append((send, recv))
        return copies

    def settle(copies):
        for send, recv in copies:
            recv.wait_recv()
        for send, recv in copies:
            send.wait_send()

    def faces(s, kind):
        low = kind == 0
        step = -1 if low else 1
        field = E if low else H
        rows = slice(0, ny) if low else slice(pad, pad + ny)
        from_x, to_x = (0, nx) if low else (nx, 0)
        idx = (ix, iy, iz)
        size = (gx, gy, gz)
        refs = (
            (field.at[s, 1:3, from_x, rows, :], field.at[s, 1:3, to_x, rows, :]),
            (ysend.at[kind, s], yrecv.at[kind, s]),
            (zsend.at[kind, s], zrecv.at[kind, s]),
        )
        out = []
        for a in range(3):
            if low:
                can_send, can_recv = idx[a] > 0, idx[a] < size[a] - 1
            else:
                can_send, can_recv = idx[a] < size[a] - 1, idx[a] > 0
            dev = [ix, iy, iz]
            dev[a] = jnp.clip(idx[a] + step, 0, size[a] - 1)
            copy = remote(refs[a][0], refs[a][1], face_send.at[kind, s, a], face_recv.at[kind, s, a], tuple(dev))
            out.append((copy, can_send, can_recv))
        return out

    def start(face, extra=None):
        copy, can_send, _ = face
        cond = can_send if extra is None else can_send & extra

        @pl.when(cond)
        def _():
            copy.start()

    def finish(face):
        copy, can_send, _ = face

        @pl.when(can_send)
        def _():
            copy.wait_send()

    def arrive(face):
        copy, _, can_recv = face

        @pl.when(can_recv)
        def _():
            copy.wait_recv()

    lane = lax.broadcasted_iota(jnp.int32, (ny, nz), 1)
    row = lax.broadcasted_iota(jnp.int32, (ny, nz), 0)

    def pack_column(acc, value, source, j):
        return jnp.where(lane == j, pltpu.roll(value, (j - source) % nz, 1), acc)

    def up_z(value, halo, j):
        return jnp.where(lane == nz - 1, pltpu.roll(halo, (nz - 1 - j) % nz, 1), pltpu.roll(value, nz - 1, 1))

    def down_z(value, halo, j):
        rolled = pltpu.roll(value, 1, 1)
        return jnp.where(lane == 0, pltpu.roll(halo, (nz - j) % nz, 1), rolled)

    def send_first(s):
        acc = jnp.zeros((ny, nz), F32)
        face = faces(s, 0)
        start(face[0])
        def planes(t, acc):
            for u in range(2):
                p = 2 * t + u
                ysend[0, s, 0, p] = E[s, 0, p, 0:1, :]
                ysend[0, s, 1, p] = E[s, 2, p, 0:1, :]
                acc = pack_column(acc, E[s, 0, p, 0:ny, :], 0, p)
                acc = pack_column(acc, E[s, 1, p, 0:ny, :], 0, nx + p)
            return acc

        acc = lax.fori_loop(0, nx // 2, planes, acc)
        zsend[0, s] = acc
        start(face[1])
        start(face[2])

    def update_h(s):
        came = faces(s, 0)
        going = faces(s, 1)
        for face in came:
            arrive(face)
        for p in range(nx):
            E[s, 0, p, ny : ny + 1, :] = yrecv[0, s, 0, p]
            E[s, 2, p, ny : ny + 1, :] = yrecv[0, s, 1, p]
        halo = zrecv[0, s]
        acc = jnp.zeros((ny, nz), F32)
        inner = slice(pad, pad + ny)
        def planes(t, acc):
            for u in range(2):
                p = nx - 1 - (2 * t + u)
                ex, ey, ez = E[s, 0, p, 0:ny, :], E[s, 1, p, 0:ny, :], E[s, 2, p, 0:ny, :]
                hx = H[s, 0, p + 1, inner, :] - HALF * (E[s, 2, p, 1 : ny + 1, :] - ez - (up_z(ey, halo, nx + p) - ey))
                hy = H[s, 1, p + 1, inner, :] - HALF * (up_z(ex, halo, p) - ex - (E[s, 2, p + 1, 0:ny, :] - ez))
                hz = H[s, 2, p + 1, inner, :] - HALF * (E[s, 1, p + 1, 0:ny, :] - ey - (E[s, 0, p, 1 : ny + 1, :] - ex))
                H[s, 0, p + 1, inner, :] = hx
                H[s, 1, p + 1, inner, :] = hy
                H[s, 2, p + 1, inner, :] = hz
                ysend[1, s, 0, p] = hx[ny - 1 : ny, :]
                ysend[1, s, 1, p] = hz[ny - 1 : ny, :]
                acc = pack_column(acc, hx, nz - 1, p)
                acc = pack_column(acc, hy, nz - 1, nx + p)

            @pl.when(t == 0)
            def _():
                start(going[0])

            return acc

        acc = lax.fori_loop(0, nx // 2, planes, acc)
        zsend[1, s] = acc
        start(going[1])
        start(going[2])

    src = src_ref[0]
    total_z, total_y = nz * gz, ny * gy
    src_i = lax.div(src, total_y * total_z) - ix * nx
    src_j = lax.rem(lax.div(src, total_z), total_y) - iy * ny
    src_k = lax.rem(src, total_z) - iz * nz
    src_mask = (row == src_j) & (lane == src_k)

    def update_e(s, k):
        came = faces(s, 1)
        going = faces(s, 0)
        for face in came:
            arrive(face)
        for face in going:
            finish(face)
        for p in range(nx):
            H[s, 0, p + 1, pad - 1 : pad, :] = yrecv[1, s, 0, p]
            H[s, 2, p + 1, pad - 1 : pad, :] = yrecv[1, s, 1, p]
        more = k < STEPS - 1
        halo = zrecv[1, s]
        acc = jnp.zeros((ny, nz), F32)
        inner = slice(pad, pad + ny)
        below = slice(pad - 1, pad + ny - 1)
        pulse = wav_ref[begin + k]
        def planes(t, acc):
            for u in range(2):
                p = 2 * t + u
                hx, hy, hz = H[s, 0, p + 1, inner, :], H[s, 1, p + 1, inner, :], H[s, 2, p + 1, inner, :]
                kp, cl = keep[p], curl[p]
                ox, oy, oz = E[s, 0, p, 0:ny, :], E[s, 1, p, 0:ny, :], E[s, 2, p, 0:ny, :]
                ex = kp * ox + cl * (hz - H[s, 2, p + 1, below, :] - (hy - down_z(hy, halo, nx + p)))
                ey = kp * oy + cl * (hx - down_z(hx, halo, p) - (hz - H[s, 2, p, inner, :]))
                ez = kp * oz + cl * (hy - H[s, 1, p, inner, :] - (hx - H[s, 0, p + 1, below, :]))
                if s == 0:
                    ez = ez + jnp.where(src_mask, jnp.where(src_i == p, pulse, 0.0), 0.0)
                    D[k, 0, p] = ex - ox
                    D[k, 1, p] = ey - oy
                    D[k, 2, p] = ez - oz
                else:
                    ez = ez + inj[k, pl.ds(pl.multiple_of(p * ny, 8), ny), :]
                    A[k, 0, p] = ex
                    A[k, 1, p] = ey
                    A[k, 2, p] = ez
                E[s, 0, p, 0:ny, :] = ex
                E[s, 1, p, 0:ny, :] = ey
                E[s, 2, p, 0:ny, :] = ez
                ysend[0, s, 0, p] = ex[0:1, :]
                ysend[0, s, 1, p] = ez[0:1, :]
                acc = pack_column(acc, ex, 0, p)
                acc = pack_column(acc, ey, 0, nx + p)

            @pl.when(t == 0)
            def _():
                start(going[0], more)

            return acc

        acc = lax.fori_loop(0, nx // 2, planes, acc)
        zsend[0, s] = acc
        start(going[1], more)
        start(going[2], more)
        for face in came_out(s):
            finish(face)

    def came_out(s):
        return faces(s, 1)

    def injection():
        cells = cells_ref[...]
        count = cells.shape[1]
        i = lax.div(cells, total_y * total_z) - ix * nx
        j = lax.rem(lax.div(cells, total_z), total_y) - iy * ny
        k = lax.rem(cells, total_z) - iz * nz
        inside = (i >= 0) & (i < nx) & (j >= 0) & (j < ny)
        where = jnp.where(inside, i * ny + j, -1)
        rows = lax.broadcasted_iota(jnp.int32, (nx * ny, count), 0)
        spots = jnp.where(rows == where, 1.0, 0.0).astype(jnp.bfloat16)
        depth = lax.broadcasted_iota(jnp.int32, (nz, count), 0) == k
        nt = (((1,), (1,)), ((), ()))
        spread_lane = lax.broadcasted_iota(jnp.int32, (nz, count), 0)
        spread_rec = lax.rem(lax.broadcasted_iota(jnp.int32, (nz, count), 1), per)
        holder = lax.div(lax.broadcasted_iota(jnp.int32, (total_devices, count), 1), per)
        holder = holder == lax.broadcasted_iota(jnp.int32, (total_devices, count), 0)
        packed = R[:, 0, :]
        for m in range(STEPS):
            spread = jnp.where(spread_lane == m * per + spread_rec, 1.0, 0.0)
            found = jnp.dot(packed, spread, precision=lax.Precision.HIGHEST, preferred_element_type=F32)
            samples = jnp.sum(jnp.where(holder, found, 0.0), axis=0, keepdims=True)
            rest = jnp.where(depth, samples, 0.0)
            total = jnp.zeros((nx * ny, nz), F32)
            for _ in range(3):
                head = rest.astype(jnp.bfloat16)
                rest = rest - head.astype(F32)
                total = total + lax.dot_general(spots, head, nt, preferred_element_type=F32)
            inj[m] = total

    loads[0].wait()
    send_first(0)
    loads[1].wait()
    send_first(1)
    gather = exchange(mine.at[0], R, g_send, g_recv)
    loads[4].wait()
    loads[5].wait()
    for p in range(nx):
        lo = loss[p]
        keep[p] = (1.0 - lo) / (1.0 + lo)
        curl[p] = 0.5 / (perm[p] * (1.0 + lo))
    loads[2].wait()
    loads[3].wait()

    update_h(0)
    update_h(1)
    update_e(0, 0)
    settle(gather)
    injection()
    update_e(1, 0)

    def body(k, carry):
        update_h(0)
        update_h(1)
        update_e(0, k)
        update_e(1, k)
        return carry

    lax.fori_loop(1, STEPS, body, 0)

    def correlate(p, squares):
        total = jnp.zeros((ny, nz), F32)
        for m in range(STEPS):
            n = STEPS - 1 - m
            total = total + (D[n, 0, p] * A[m, 0, p] + D[n, 1, p] * A[m, 1, p] + D[n, 2, p] * A[m, 2, p])
        g = -total / perm[p]
        grad[p] = g
        return squares + g * g

    squares = lax.fori_loop(0, nx, correlate, jnp.zeros((ny, nz), F32))
    part[0] = jnp.sum(squares, axis=0, keepdims=True)
    sums[pl.ds(me, 1)] = part[...]
    settle(exchange(part.at[0], sums, r_send, r_recv))
    tile = sums[:, 0, :]
    total = jnp.sum(jnp.sum(tile, axis=0, keepdims=True), axis=1, keepdims=True)
    rms = jnp.sqrt(total / (nx * ny * nz * gx * gy * gz) + 1e-06)
    rms_ref[...] = rms
    inverse = 1.0 / rms
    for p in range(nx):
        out_ref[p] = grad[p] * inverse


def per_device(
    permittivity, loss, fwd_electric, fwd_magnetic, adj_electric, adj_magnetic,
    wavelet, residuals, source_cell, receiver_cells, start_step,
):
    sizes = tuple(lax.axis_size(a) for a in ("gx", "gy", "gz"))
    gx, gy, gz = sizes
    nx, ny, nz = permittivity.shape
    devices = gx * gy * gz
    count = receiver_cells.shape[0]
    vmem = pl.BlockSpec(memory_space=pltpu.VMEM)
    hbm = pl.BlockSpec(memory_space=pltpu.HBM)
    dma = pltpu.SemaphoreType.DMA
    block = (nx, ny, nz)
    padded = (2, 3, nx + 1, ny + 8, nz)
    direction, rms = pl.pallas_call(
        functools.partial(kernel, sizes),
        out_shape=(
            pltpu.VMEM(block, F32),
            jax.ShapeDtypeStruct((1, 1), F32),
        ),
        in_specs=[hbm] * 11,
        out_specs=(vmem, vmem),
        scratch_shapes=[
            pltpu.VMEM(padded, F32),
            pltpu.VMEM(padded, F32),
            pltpu.VMEM(block, F32),
            pltpu.VMEM(block, F32),
            pltpu.VMEM(block, F32),
            pltpu.VMEM(block, F32),
            pltpu.VMEM((STEPS, 3) + block, F32),
            pltpu.VMEM((STEPS, 3) + block, F32),
            pltpu.VMEM((STEPS, nx * ny, nz), F32),
            pltpu.VMEM((devices, 1, nz), F32),
            pltpu.VMEM(block, F32),
            pltpu.VMEM((2, 2, 2, nx, 1, nz), F32),
            pltpu.VMEM((2, 2, 2, nx, 1, nz), F32),
            pltpu.VMEM((2, 2, ny, nz), F32),
            pltpu.VMEM((2, 2, ny, nz), F32),
            pltpu.VMEM((1, 1, nz), F32),
            pltpu.VMEM((devices, 1, nz), F32),
            pltpu.SMEM(wavelet.shape, F32),
            pltpu.SMEM((1,), jnp.int32),
            pltpu.SMEM((1,), jnp.int32),
            pltpu.VMEM((1, count), jnp.int32),
            pltpu.VMEM(residuals.shape, F32),
            pltpu.VMEM((1, 1, nz), F32),
            dma((11,)),
            dma((2, 2, 3)),
            dma((2, 2, 3)),
            dma((devices,)),
            dma((devices,)),
            dma((devices,)),
            dma((devices,)),
        ],
        compiler_params=pltpu.CompilerParams(
            collective_id=0, has_side_effects=True, vmem_limit_bytes=60 * 1024 * 1024
        ),
    )(
        wavelet, source_cell, start_step, receiver_cells.reshape(1, count),
        permittivity, loss, fwd_electric, fwd_magnetic, adj_electric, adj_magnetic, residuals,
    )
    return direction, rms.reshape(())


def solution(mesh):
    block = P("gx", "gy", "gz")
    state = P(None, "gx", "gy", "gz")
    return jax.shard_map(
        per_device,
        mesh=mesh,
        in_specs=(
            block, block, state, state, state, state,
            P(), P(("gx", "gy", "gz"), None), P(), P(), P(),
        ),
        out_specs=(block, P()),
        check_vma=False,
    )
```
